32 devices in a mesh: parts: 2 (over x), seq: 16 (over z, y, core).
Axes of the slice: x: 2, y: 2, z: 4, core: 2. Of those that a mesh axis runs over, the one named last changes fastest.
Arguments:
- token_ids: int32 [4, 4], P(None, 'parts'), parts along dimension 1, may hold values from 0 to 76031
- lengths: int32 [4], P('parts'), parts along dimension 0, may hold values from 24576 to 32768, as said below
- embed_table: bfloat16 [76032, 5120], P('seq'), may hold values from -6 to 6
- attn_gain: bfloat16 [5120], replicated, may hold values from 0.25 to 1.75
- w_qkv: bfloat16 [5120, 7168], P('seq'), may hold values from -0.125 to 0.125
- qkv_bias: float32 [7168], replicated, may hold values from -8 to 8
- cache_keys: bfloat16 [4, 32768, 1024], P('parts', 'seq'), parts along dimension 0, may hold values from -300 to 300
- cache_values: bfloat16 [4, 32768, 1024], P('parts', 'seq'), parts along dimension 0, may hold values from -6 to 6
- w_out: bfloat16 [5120, 5120], P(None, 'seq'), may hold values from -0.078125 to 0.078125
- mlp_gain: bfloat16 [5120], replicated, may hold values from 0.25 to 1.75
- w_gate: bfloat16 [5120, 16384], P(None, 'seq'), may hold values from -0.078125 to 0.078125
- w_up: bfloat16 [5120, 16384], P(None, 'seq'), may hold values from -0.078125 to 0.078125
- w_down: bfloat16 [16384, 5120], P('seq'), may hold values from -0.0625 to 0.0625
Outputs:
- attended: bfloat16 [4, 4, 5120], P(None, 'parts'), parts along dimension 1
- layer_out: bfloat16 [4, 4, 5120], P(None, 'parts', 'seq'), parts along dimension 1
The draws below stay inside these ranges and needn't reach their ends.
There are 2 independent parts, one for each index of `parts`. The reference program is written for one: setup_inputs(seed, part) draws one part's arguments, and reference() takes and returns one part's arrays. A program takes and returns all parts, laid end to end along the dimension named above; an argument that names none is the same for every part. Nothing has to cross between parts.
Inputs may be any that keep to these rules, and one draw needn't show every extreme that they name: Cache positions lengths[b] and later are unused; the first prompt fills the whole cache of 32768 positions.
All inputs are finite; a program needn't handle non-finite values.
Results may differ from the reference program's by a relative error of at most 0.017.
The reference program's roundings to bfloat16 on the way (of `normed`, `joint`, `normed_mid` and `hidden`) count: a program that leaves them out, or rounds other values in their place, can miss the bound.
Values may be sent and summed in bfloat16 or wider, within the bound.
A program may use at most 192 MiB of HBM per device.

```python
import jax
import jax.numpy as jnp
from jax import lax

D = 5120
HEADS = 40
KV_HEADS = 8
HEAD_DIM = 128
FF = 16384
VOCAB = 76032
CTX = 32768
STEPS = 4
SEQS = 2
QD = 5120
KVD = 1024
QKV = 7168


def draw_lengths(key, part):
    drawn = jax.random.randint(jax.random.fold_in(key, 3), (SEQS,), CTX - CTX // 4, CTX + 1, dtype=jnp.int32)
    return drawn.at[0].set(CTX)


def draw_qkv_bias(key, part):
    key_one, key_two, key_three, key_four = jax.random.split(jax.random.fold_in(key, 11), 4)
    direction = jax.random.normal(key_one, (KV_HEADS, HEAD_DIM), jnp.float32)
    strength = jax.random.uniform(key_two, (KV_HEADS, 1), jnp.float32, 1.05, 1.3)
    aligned = direction * strength
    query_noise = 0.5 * jax.random.normal(key_three, (KV_HEADS, HEADS // KV_HEADS, HEAD_DIM), jnp.float32)
    query_part = (aligned[:, None, :] + query_noise).reshape(HEADS * HEAD_DIM)
    key_part = aligned.reshape(KV_HEADS * HEAD_DIM)
    value_part = 0.5 * jax.random.normal(key_four, (KV_HEADS * HEAD_DIM,), jnp.float32)
    joined = jnp.concatenate([query_part, key_part, value_part])
    return jnp.clip(joined, -8.0, 8.0)


def draw_cache_keys(key, part):
    key_one = jax.random.fold_in(jax.random.fold_in(key, 17), 0)
    base = 2.2 * jax.random.normal(key_one, (SEQS, CTX, KV_HEADS, HEAD_DIM), jnp.float32)
    return jnp.clip(base, -300.0, 300.0).reshape(SEQS, CTX, KV_HEADS * HEAD_DIM).astype(jnp.bfloat16)


def touch_ends(entries, key, low, largest):
    dims = entries.shape
    index_at = [jax.random.randint(jax.random.fold_in(key, axis), (), 0, dims[axis]) for axis in range(len(dims))]
    entries = entries.at[tuple(index_at)].set(low)
    longest = dims.index(max(dims))
    index_at[longest] = (index_at[longest] + 1) % dims[longest]
    return entries.at[tuple(index_at)].set(largest)


def spiked(values, rng, source, target, parts, factor):
    def block_of(dim):
        return (jnp.arange(values.shape[dim]) // (values.shape[dim] // parts)).reshape((-1,) + (1,) * (values.ndim - 1 - dim))

    first = jax.random.permutation(rng, parts)[block_of(target)]
    far = (block_of(target) + parts // 2) % parts
    return jnp.where((block_of(source) == first) | (block_of(source) == far), factor * values, values)


def level_of(rng, shape, shards, smallest, top_value):
    level, own = 1.0, jax.random.fold_in(rng, 6)
    for dim, parts in shards:
        steps = jnp.exp(jax.random.uniform(jax.random.fold_in(own, dim), (parts,), jnp.float32, smallest / len(shards), top_value / len(shards)))
        level = level * jnp.repeat(steps, shape[dim] // parts).reshape([-1 if axis == dim else 1 for axis in range(len(shape))])
    return level


def gaussian(key, shape, spread, most, pieces=(), held_as=jnp.bfloat16):
    values = jax.random.normal(key, shape, jnp.float32) * spread
    if len(pieces) > 0:
        values = level_of(key, shape, pieces, -0.22, 0.18) * values
    return jnp.clip(values, min=-most, max=most).astype(held_as)


def heavy_noise(own_key, shape, spread, most, shards, heavy, held_as=jnp.bfloat16):
    entries = spread * jax.random.normal(own_key, shape, jnp.float32)
    if shards:
        entries = entries * level_of(own_key, shape, shards, -0.22, 0.18)
    return jnp.clip(spiked(entries, jax.random.fold_in(own_key, 3), *heavy), -most, most).astype(held_as)


def setup_inputs(seed: int = 0, part: int = 0) -> dict:
    streams_of = jax.random.split(jax.random.key(seed), 14)
    part_keys = jax.random.split(jax.random.fold_in(streams_of[13], part), 14)
    token_ids = touch_ends(jax.random.randint(part_keys[0], (STEPS, SEQS), 0, VOCAB), jax.random.fold_in(part_keys[0], 1), 0, VOCAB - 1).astype(jnp.int32)
    lengths = draw_lengths(jax.random.fold_in(jax.random.fold_in(streams_of[13], part), 71), part)
    embed_table = gaussian(streams_of[2], (VOCAB, D), 0.5, 6.0, ((0, 16),))
    attn_gain = jnp.clip(1.0 + 0.15 * jax.random.normal(streams_of[3], (D,), jnp.float32), 0.25, 1.75).astype(jnp.bfloat16)
    w_qkv = heavy_noise(streams_of[4], (D, QKV), D ** -0.5, 0.125, ((0, 16),), (0, 1, 16, 2.0))
    qkv_bias = draw_qkv_bias(jax.random.fold_in(streams_of[13], 71), part)
    cache_keys = draw_cache_keys(jax.random.fold_in(jax.random.fold_in(streams_of[13], part), 71), part)
    cache_values = gaussian(part_keys[7], (SEQS, CTX, KVD), 1.0, 6.0, ((1, 16),))
    w_out = gaussian(streams_of[8], (QD, D), QD ** -0.5, 0.078125, ((1, 16),))
    mlp_gain = jnp.clip(1.0 + 0.15 * jax.random.normal(streams_of[9], (D,), jnp.float32), 0.25, 1.75).astype(jnp.bfloat16)
    w_gate = gaussian(streams_of[10], (D, FF), D ** -0.5, 0.078125, ((1, 16),))
    w_up = gaussian(streams_of[11], (D, FF), D ** -0.5, 0.078125, ((1, 16),))
    w_down = heavy_noise(streams_of[12], (FF, D), FF ** -0.5, 0.0625, ((0, 16),), (0, 1, 16, 2.0))
    return {"token_ids": token_ids, "lengths": lengths, "embed_table": embed_table, "attn_gain": attn_gain, "w_qkv": w_qkv, "qkv_bias": qkv_bias, "cache_keys": cache_keys, "cache_values": cache_values, "w_out": w_out, "mlp_gain": mlp_gain, "w_gate": w_gate, "w_up": w_up, "w_down": w_down}


NORM_EPS = 1e-06
ROPE_BASE = 1000000.0
MASKED = -1e+30

def rms_normalize(rows, gain):
    mean_square = lax.optimization_barrier(jnp.mean(rows * rows, axis=-1, keepdims=True))
    return (rows * lax.rsqrt(mean_square + NORM_EPS) * gain.astype(jnp.float32)).astype(jnp.bfloat16)

def rotate(vectors, positions):
    half_dim = vectors.shape[-1] // 2
    frequency = ROPE_BASE ** (-2.0 * jnp.arange(half_dim, dtype=jnp.float32) / vectors.shape[-1])
    angles = positions.astype(jnp.float32)[..., None, None] * frequency
    cosine = jnp.cos(angles)
    sine_part = jnp.sin(angles)
    widened = vectors.astype(jnp.float32)
    first_half = widened[..., :half_dim]
    second = widened[..., half_dim:]
    joined = jnp.concatenate([first_half * cosine - second * sine_part, second * cosine + first_half * sine_part], axis=-1)
    return joined.astype(jnp.bfloat16)

def attend_one(query_rows, key_rows, value_rows, cached_keys, cached_values, length):
    all_keys = jnp.concatenate([cached_keys.reshape(CTX, KV_HEADS, HEAD_DIM), key_rows], axis=0).astype(jnp.float32)
    all_values = jnp.concatenate([cached_values.reshape(CTX, KV_HEADS, HEAD_DIM), value_rows], axis=0).astype(jnp.float32)
    grouped = query_rows.reshape(STEPS, KV_HEADS, HEADS // KV_HEADS, HEAD_DIM).astype(jnp.float32)
    scores = jnp.einsum('skgd,pkd->kgsp', grouped, all_keys) * HEAD_DIM ** (-0.5)
    places = jnp.arange(CTX + STEPS, dtype=jnp.int32)
    step_index = jnp.arange(STEPS, dtype=jnp.int32)
    cache_valid = places[None, :] < length
    new_valid = places[None, :] - CTX <= step_index[:, None]
    valid = jnp.where(places[None, :] < CTX, cache_valid, new_valid)
    masked = jnp.where(valid, scores, MASKED)
    top_score = lax.optimization_barrier(jnp.max(masked, axis=-1, keepdims=True))
    weights = jnp.where(valid, jnp.exp(masked - top_score), 0.0)
    total = lax.optimization_barrier(jnp.sum(weights, axis=-1))
    rounded = lax.optimization_barrier(weights.astype(jnp.bfloat16)).astype(jnp.float32)
    summed = jnp.einsum('kgsp,pkd->kgsd', rounded, all_values)
    result = summed / total[..., None]
    result = jnp.transpose(result, (2, 0, 1, 3))
    return result.reshape(STEPS, HEADS * HEAD_DIM).astype(jnp.bfloat16)

def reference(token_ids, lengths, embed_table, attn_gain, w_qkv, qkv_bias, cache_keys, cache_values, w_out, mlp_gain, w_gate, w_up, w_down):
    query_width = HEADS * HEAD_DIM
    key_width = KV_HEADS * HEAD_DIM
    stream = embed_table[token_ids].astype(jnp.float32)
    normed = rms_normalize(stream, attn_gain)
    joint = jnp.dot(normed.reshape(-1, D), w_qkv, preferred_element_type=jnp.float32) + qkv_bias.astype(jnp.float32)
    joint = joint.astype(jnp.bfloat16).reshape(STEPS, SEQS, -1)
    query_part = joint[..., :query_width].reshape(STEPS, SEQS, HEADS, HEAD_DIM)
    key_part = joint[..., query_width:query_width + key_width].reshape(STEPS, SEQS, KV_HEADS, HEAD_DIM)
    value_part = joint[..., query_width + key_width:].reshape(STEPS, SEQS, KV_HEADS, HEAD_DIM)
    positions = lengths[None, :] + jnp.arange(STEPS, dtype=jnp.int32)[:, None]
    queries = rotate(query_part, positions)
    new_keys = rotate(key_part, positions)
    outputs = []
    for seq_index in range(SEQS):
        outputs.append(attend_one(queries[:, seq_index], new_keys[:, seq_index], value_part[:, seq_index], cache_keys[seq_index], cache_values[seq_index], lengths[seq_index]))
    attended = jnp.stack(outputs, axis=1)
    projected = jnp.dot(attended.reshape(-1, query_width), w_out, preferred_element_type=jnp.float32)
    mid = stream + projected.reshape(STEPS, SEQS, D)
    normed_mid = rms_normalize(mid, mlp_gain).reshape(-1, D)
    gate = jnp.dot(normed_mid, w_gate, preferred_element_type=jnp.float32)
    upper = jnp.dot(normed_mid, w_up, preferred_element_type=jnp.float32)
    hidden = (jax.nn.silu(gate) * upper).astype(jnp.bfloat16)
    down = jnp.dot(hidden, w_down, preferred_element_type=jnp.float32).reshape(STEPS, SEQS, D)
    layer_out = (mid + down).astype(jnp.bfloat16)
    return (attended, layer_out)
```

```python
import functools
import math

import jax
import jax.numpy as jnp
from jax import lax
from jax.experimental import pallas as pl
from jax.experimental.pallas import tpu as pltpu
from jax.sharding import PartitionSpec as P

HEADS = 40
KV_HEADS = 8
HEAD_DIM = 128

NORM_EPS = 1e-06
ROPE_BASE = 1000000.0
MASKED = -1e30
F32 = jnp.float32
BF16 = jnp.bfloat16
MESH = pl.DeviceIdType.MESH


def layer_kernel(
    n,
    lengths,
    picked,
    inside,
    gain_one,
    bias,
    cos,
    sin,
    gain_two,
    qkv_hbm,
    keys_hbm,
    values_hbm,
    out_hbm,
    gate_hbm,
    up_hbm,
    down_hbm,
    attended_ref,
    layer_ref,
    w_qkv,
    keys,
    values,
    w_out,
    w_gate,
    w_up,
    w_down,
    rows_out,
    rows_in,
    joint_out,
    joint_in,
    heads_all,
    heads_wide,
    part_out,
    part_in,
    attended_all,
    mid_all,
    wide,
    narrow,
    down_out,
    down_in,
    load_sem,
    send_sem,
    recv_sem,
):
    me = lax.axis_index("seq")
    group = HEADS // KV_HEADS
    joint_heads = HEADS + 2 * KV_HEADS
    tokens, width = picked.shape
    batches = keys.shape[0]
    local_len = keys.shape[1]
    cols = w_out.shape[1]
    joint_each = joint_out.shape[1]
    head_each = part_out.shape[1] - 1
    scale = 1.0 / math.sqrt(HEAD_DIM)

    loads = [
        pltpu.make_async_copy(a, b, load_sem.at[i])
        for i, (a, b) in enumerate(
            (
                (qkv_hbm, w_qkv),
                (keys_hbm, keys),
                (values_hbm, values),
                (out_hbm, w_out),
                (gate_hbm, w_gate),
                (up_hbm, w_up),
                (down_hbm, w_down),
            )
        )
    ]
    for load in loads:
        load.start()

    barrier = pltpu.get_barrier_semaphore()

    @pl.loop(1, n)
    def _(d):
        pl.semaphore_signal(
            barrier, inc=1, device_id={"seq": lax.rem(me + d, n)}, device_id_type=MESH
        )

    def copy_to(step, source, target, slot, peer):
        return pltpu.make_async_remote_copy(
            src_ref=source,
            dst_ref=target.at[slot],
            send_sem=send_sem.at[step, peer],
            recv_sem=recv_sem.at[step, slot],
            device_id={"seq": peer},
            device_id_type=MESH,
        )

    def send_all(step, source, target, spread):
        @pl.loop(1, n)
        def _(d):
            peer = lax.rem(me + d, n)
            copy_to(step, source.at[peer if spread else me], target, me, peer).start()

    def receive_all(step, target):
        @pl.loop(1, n)
        def _(d):
            peer = lax.rem(me + d, n)
            copy_to(step, target.at[peer], target, peer, peer).wait_recv()

    def sent_all(step, source, spread):
        @pl.loop(1, n)
        def _(d):
            peer = lax.rem(me + d, n)
            src = source.at[peer if spread else me]
            pltpu.make_async_remote_copy(
                src_ref=src,
                dst_ref=src,
                send_sem=send_sem.at[step, peer],
                recv_sem=recv_sem.at[step, peer],
                device_id={"seq": peer},
                device_id_type=MESH,
            ).wait_send()

    wide[...] = picked[...].astype(F32) * inside[...]
    mean_square = jnp.sum(wide[...] * wide[...], axis=1, keepdims=True) / width
    normed = (wide[...] * lax.rsqrt(mean_square + NORM_EPS) * gain_one[...]).astype(BF16)
    heads_out = jnp.concatenate([wide[...], normed.astype(F32)], axis=0)
    for j in range(n):
        rows_out[j] = heads_out[:, j * cols : (j + 1) * cols].astype(BF16)
    part_out[...] = jnp.zeros_like(part_out)
    pl.semaphore_wait(barrier, n - 1)
    send_all(0, rows_out, rows_in, True)
    rows_in[me] = rows_out[me]
    receive_all(0, rows_in)
    rows = lax.fori_loop(
        1, n, lambda j, acc: acc + rows_in[j].astype(F32), rows_in[0].astype(F32)
    )
    stream = rows[:tokens]
    normed_local = rows[tokens:].astype(BF16)

    loads[0].wait()
    chunk = 4

    @pl.loop(0, joint_heads // chunk)
    def _(c):
        part = jnp.dot(
            normed_local,
            w_qkv[:, pl.ds(pl.multiple_of(c * (chunk * HEAD_DIM), HEAD_DIM), chunk * HEAD_DIM)],
            preferred_element_type=F32,
        )
        for i in range(chunk):
            h = c * chunk + i
            joint_out[h // joint_each, h % joint_each] = part[:, i * HEAD_DIM : (i + 1) * HEAD_DIM]

    for h in range(joint_heads, n * joint_each):
        joint_out[h // joint_each, h % joint_each] = jnp.zeros((tokens, HEAD_DIM), F32)
    send_all(1, joint_out, joint_in, True)
    joint_in[me] = joint_out[me]
    receive_all(1, joint_in)
    joint = lax.fori_loop(1, n, lambda j, acc: acc + joint_in[j], joint_in[0])
    tiles = []
    for i in range(joint_each):
        h = jnp.minimum(me * joint_each + i, joint_heads - 1)
        x = (joint[i] + bias[pl.ds(h, 1), :]).astype(BF16).astype(F32)
        turned = x * cos[...] + pltpu.roll(x, HEAD_DIM // 2, 1) * sin[...]
        is_key = jnp.full(x.shape, h, jnp.int32) < HEADS + KV_HEADS
        tiles.append(jnp.where(is_key, turned, x))
    heads_all[me] = jnp.concatenate(tiles, axis=0).astype(BF16)
    send_all(2, heads_all, heads_all, False)
    receive_all(2, heads_all)
    rows_each = joint_each * tokens

    @pl.loop(0, n)
    def _(j):
        heads_wide[pl.ds(pl.multiple_of(j * rows_each, 8), rows_each), :] = heads_all[j].astype(F32)

    loads[1].wait()
    loads[2].wait()
    group_rows = group * tokens
    row_batch = lax.broadcasted_iota(jnp.int32, (group_rows, 1), 0) % batches
    places = me * local_len + lax.broadcasted_iota(jnp.int32, (1, local_len), 1)
    lane = lax.broadcasted_iota(jnp.int32, (tokens, HEAD_DIM), 1)

    @pl.loop(0, KV_HEADS)
    def _(k):
        q = heads_wide[pl.ds(pl.multiple_of(k * group_rows, 8), group_rows), :].astype(BF16)
        head_cols = pl.ds(pl.multiple_of(k * HEAD_DIM, HEAD_DIM), HEAD_DIM)
        top = total = summed = None
        for b in range(batches):
            valid = places < lengths[b]
            scores = lax.dot_general(
                q, keys[b, :, head_cols], (((1,), (1,)), ((), ())), preferred_element_type=F32
            )
            masked = jnp.where(valid, scores * scale, MASKED)
            own_top = jnp.max(masked, axis=1, keepdims=True)
            weight = jnp.where(valid, jnp.exp(masked - own_top), 0.0)
            own_total = jnp.sum(weight, axis=1, keepdims=True)
            own_sum = jnp.dot(
                weight.astype(BF16), values[b, :, head_cols], preferred_element_type=F32
            )
            if b == 0:
                top, total, summed = own_top, own_total, own_sum
            else:
                here = row_batch == b
                top = jnp.where(here, own_top, top)
                total = jnp.where(here, own_total, total)
                summed = jnp.where(here, own_sum, summed)
        for g in range(group):
            h = k * group + g
            owner, slot = h // head_each, h % head_each
            mine = slice(g * tokens, (g + 1) * tokens)
            part_out[owner, slot] = summed[mine]
            stats = part_out[owner, head_each]
            stats = jnp.where(lane == 2 * slot, top[mine], stats)
            part_out[owner, head_each] = jnp.where(lane == 2 * slot + 1, total[mine], stats)

    send_all(3, part_out, part_in, True)
    part_in[me] = part_out[me]

    row = lax.broadcasted_iota(jnp.int32, (tokens, 1), 0)
    fresh = []
    for i in range(head_each):
        h = jnp.minimum(me * head_each + i, HEADS - 1)
        kv = h // group
        q = heads_wide[pl.ds(pl.multiple_of(h * tokens, 8), tokens), :]
        new_key = heads_wide[pl.ds(pl.multiple_of((HEADS + kv) * tokens, 8), tokens), :]
        new_value = heads_wide[
            pl.ds(pl.multiple_of((HEADS + KV_HEADS + kv) * tokens, 8), tokens), :
        ]
        scores = []
        top = jnp.full((tokens, 1), MASKED, F32)
        for t in range(tokens):
            seen = (row % batches == t % batches) & (row >= t)
            score = jnp.sum(q * new_key[t : t + 1], axis=1, keepdims=True) * scale
            score = jnp.where(seen, score, MASKED)
            scores.append((seen, score))
            top = jnp.maximum(top, score)
        fresh.append((top, scores, new_value))

    receive_all(3, part_in)
    tiles = []
    for i in range(head_each):
        top, scores, new_value = fresh[i]

        def stat(j, which):
            return jnp.broadcast_to(
                part_in[j, head_each][:, 2 * i + which : 2 * i + which + 1], (tokens, HEAD_DIM)
            )

        top = jnp.broadcast_to(top, (tokens, HEAD_DIM))
        top = lax.fori_loop(0, n, lambda j, m: jnp.maximum(m, stat(j, 0)), top)
        total = jnp.zeros((tokens, HEAD_DIM), F32)
        summed = jnp.zeros((tokens, HEAD_DIM), F32)
        for t in range(tokens):
            seen, score = scores[t]
            weight = jnp.where(seen, jnp.exp(score - top), 0.0)
            total += weight
            summed += weight.astype(BF16).astype(F32) * new_value[t : t + 1]

        def merge(j, state):
            total, summed = state
            factor = jnp.exp(stat(j, 0) - top)
            return total + stat(j, 1) * factor, summed + part_in[j, i] * factor

        total, summed = lax.fori_loop(0, n, merge, (total, summed))
        tiles.append(summed / total)
    attended_all[me] = jnp.concatenate(tiles, axis=0).astype(BF16)
    send_all(4, attended_all, attended_all, False)
    receive_all(4, attended_all)
    for h in range(HEADS):
        at = (h % head_each) * tokens
        wide[:, h * HEAD_DIM : (h + 1) * HEAD_DIM] = attended_all[h // head_each].astype(F32)[
            at : at + tokens
        ]
    narrow[...] = wide[...].astype(BF16)
    attended_ref[...] = narrow[...]

    loads[3].wait()
    depth = 512

    def piece(c):
        return pl.ds(pl.multiple_of(c * depth, depth), depth)

    mid = stream + lax.fori_loop(
        0,
        width // depth,
        lambda c, acc: acc
        + jnp.dot(narrow[:, piece(c)], w_out[piece(c), :], preferred_element_type=F32),
        jnp.zeros((tokens, cols), F32),
    )
    mid_all[me] = mid
    send_all(5, mid_all, mid_all, False)
    receive_all(5, mid_all)
    for j in range(n):
        wide[:, j * cols : (j + 1) * cols] = mid_all[j]
    mean_square = jnp.sum(wide[...] * wide[...], axis=1, keepdims=True) / width
    narrow[...] = (wide[...] * lax.rsqrt(mean_square + NORM_EPS) * gain_two[...]).astype(BF16)

    loads[4].wait()
    loads[5].wait()
    units = w_gate.shape[1]

    def both(c, state):
        gate, upper = state
        x = narrow[:, piece(c)]
        return (
            gate + jnp.dot(x, w_gate[piece(c), :], preferred_element_type=F32),
            upper + jnp.dot(x, w_up[piece(c), :], preferred_element_type=F32),
        )

    zero = jnp.zeros((tokens, units), F32)
    gate, upper = lax.fori_loop(0, width // depth, both, (zero, zero))
    hidden = (gate / (1.0 + jnp.exp(-gate)) * upper).astype(BF16)
    loads[6].wait()

    @pl.loop(0, width // depth)
    def _(c):
        wide[:, piece(c)] = jnp.dot(hidden, w_down[:, piece(c)], preferred_element_type=F32)

    for j in range(n):
        down_out[j] = wide[:, j * cols : (j + 1) * cols]
    send_all(6, down_out, down_in, True)
    down_in[me] = down_out[me]
    receive_all(6, down_in)
    summed = lax.fori_loop(1, n, lambda j, acc: acc + down_in[j], down_in[0])
    layer_ref[...] = (mid + summed).astype(BF16)

    sent_all(0, rows_out, True)
    sent_all(1, joint_out, True)
    sent_all(2, heads_all, False)
    sent_all(3, part_out, True)
    sent_all(4, attended_all, False)
    sent_all(5, mid_all, False)
    sent_all(6, down_out, True)


def body(
    token_ids,
    lengths,
    embed_table,
    attn_gain,
    w_qkv,
    qkv_bias,
    cache_keys,
    cache_values,
    w_out,
    mlp_gain,
    w_gate,
    w_up,
    w_down,
):
    n = lax.axis_size("seq")
    rank = lax.axis_index("seq")
    step_count, batch_count = token_ids.shape
    tokens = step_count * batch_count
    width = embed_table.shape[1]
    vocab_rows = embed_table.shape[0]
    cols = w_out.shape[1]
    local_ids = token_ids.reshape(-1) - rank * vocab_rows
    inside = (local_ids >= 0) & (local_ids < vocab_rows)
    picked = embed_table.at[jnp.clip(local_ids, 0, vocab_rows - 1)].get(mode="promise_in_bounds")
    positions = (lengths[None, :] + jnp.arange(step_count, dtype=jnp.int32)[:, None]).reshape(-1)
    half = HEAD_DIM // 2
    frequency = ROPE_BASE ** (-2.0 * jnp.arange(half, dtype=F32) / HEAD_DIM)
    angles = positions.astype(F32)[:, None] * frequency
    cosine, sine = jnp.cos(angles), jnp.sin(angles)
    cos = jnp.concatenate([cosine, cosine], axis=1)
    sin = jnp.concatenate([-sine, sine], axis=1)
    joint_heads = HEADS + 2 * KV_HEADS
    joint_each = -(-joint_heads // n)
    head_each = -(-HEADS // n)
    vmem = pl.BlockSpec(memory_space=pltpu.VMEM)
    hbm = pl.BlockSpec(memory_space=pl.ANY)
    attended, layer_out = pl.pallas_call(
        functools.partial(layer_kernel, n),
        out_shape=(
            jax.ShapeDtypeStruct((tokens, width), BF16),
            jax.ShapeDtypeStruct((tokens, cols), BF16),
        ),
        in_specs=[pl.BlockSpec(memory_space=pltpu.SMEM)] + [vmem] * 7 + [hbm] * 7,
        out_specs=(vmem, vmem),
        scratch_shapes=[
            pltpu.VMEM(a.shape, a.dtype)
            for a in (w_qkv, cache_keys, cache_values, w_out, w_gate, w_up, w_down)
        ]
        + [
            pltpu.VMEM((n, 2 * tokens, cols), BF16),
            pltpu.VMEM((n, 2 * tokens, cols), BF16),
            pltpu.VMEM((n, joint_each, tokens, HEAD_DIM), F32),
            pltpu.VMEM((n, joint_each, tokens, HEAD_DIM), F32),
            pltpu.VMEM((n, joint_each * tokens, HEAD_DIM), BF16),
            pltpu.VMEM((n * joint_each * tokens, HEAD_DIM), F32),
            pltpu.VMEM((n, head_each + 1, tokens, HEAD_DIM), F32),
            pltpu.VMEM((n, head_each + 1, tokens, HEAD_DIM), F32),
            pltpu.VMEM((n, head_each * tokens, HEAD_DIM), BF16),
            pltpu.VMEM((n, tokens, cols), F32),
            pltpu.VMEM((tokens, width), F32),
            pltpu.VMEM((tokens, width), BF16),
            pltpu.VMEM((n, tokens, cols), F32),
            pltpu.VMEM((n, tokens, cols), F32),
            pltpu.SemaphoreType.DMA((7,)),
            pltpu.SemaphoreType.DMA((7, n)),
            pltpu.SemaphoreType.DMA((7, n)),
        ],
        compiler_params=pltpu.CompilerParams(
            collective_id=0, has_side_effects=True, vmem_limit_bytes=67043328
        ),
    )(
        lengths,
        picked,
        inside.astype(F32)[:, None],
        attn_gain.astype(F32)[None, :],
        qkv_bias.reshape(joint_heads, HEAD_DIM),
        cos,
        sin,
        mlp_gain.astype(F32)[None, :],
        w_qkv,
        cache_keys,
        cache_values,
        w_out,
        w_gate,
        w_up,
        w_down,
    )
    return (
        attended.reshape(step_count, batch_count, width),
        layer_out.reshape(step_count, batch_count, cols),
    )


def solution(mesh):
    return jax.shard_map(
        body,
        mesh=mesh,
        in_specs=(
            P(None, "parts"),
            P("parts"),
            P("seq", None),
            P(),
            P("seq", None),
            P(),
            P("parts", "seq", None),
            P("parts", "seq", None),
            P(None, "seq"),
            P(),
            P(None, "seq"),
            P(None, "seq"),
            P("seq", None),
        ),
        out_specs=(P(None, "parts", None), P(None, "parts", "seq")),
        check_vma=False,
    )
```

```python
import functools
import math

import jax
import jax.numpy as jnp
from jax import lax
from jax.experimental import pallas as pl
from jax.experimental.pallas import tpu as pltpu
from jax.sharding import PartitionSpec as P

HEADS = 40
KV_HEADS = 8
HEAD_DIM = 128

NORM_EPS = 1e-06
ROPE_BASE = 1000000.0
MASKED = -1e30
F32 = jnp.float32
BF16 = jnp.bfloat16
MESH = pl.DeviceIdType.MESH


def layer_kernel(
    n,
    lengths,
    picked,
    inside,
    gain_one,
    bias,
    cos,
    sin,
    gain_two,
    qkv_hbm,
    keys_hbm,
    values_hbm,
    out_hbm,
    gate_hbm,
    up_hbm,
    down_hbm,
    attended_ref,
    layer_ref,
    w_qkv,
    keys,
    values,
    w_out,
    w_gate,
    w_up,
    w_down,
    rows_out,
    rows_in,
    joint_out,
    joint_in,
    heads_all,
    heads_wide,
    part_out,
    part_in,
    attended_all,
    mid_all,
    wide,
    narrow,
    down_out,
    down_in,
    group_sum,
    group_top,
    group_total,
    load_sem,
    send_sem,
    recv_sem,
):
    me = lax.axis_index("seq")
    group = HEADS // KV_HEADS
    joint_heads = HEADS + 2 * KV_HEADS
    tokens, width = picked.shape
    batches = keys.shape[0]
    local_len = keys.shape[1]
    cols = w_out.shape[0]
    joint_each = joint_out.shape[1]
    head_each = part_out.shape[1] - 1
    scale = 1.0 / math.sqrt(HEAD_DIM)

    loads = [
        pltpu.make_async_copy(a, b, load_sem.at[i])
        for i, (a, b) in enumerate(
            (
                (qkv_hbm, w_qkv),
                (keys_hbm, keys),
                (values_hbm, values),
                (out_hbm, w_out),
                (gate_hbm, w_gate),
                (up_hbm, w_up),
                (down_hbm, w_down),
            )
        )
    ]
    for load in loads:
        load.start()

    barrier = pltpu.get_barrier_semaphore()

    @pl.loop(1, n)
    def _(d):
        pl.semaphore_signal(
            barrier, inc=1, device_id={"seq": lax.rem(me + d, n)}, device_id_type=MESH
        )

    def copy_to(step, source, target, slot, peer):
        return pltpu.make_async_remote_copy(
            src_ref=source,
            dst_ref=target.at[slot],
            send_sem=send_sem.at[step, peer],
            recv_sem=recv_sem.at[step, slot],
            device_id={"seq": peer},
            device_id_type=MESH,
        )

    def send_all(step, source, target, spread):
        @pl.loop(1, n)
        def _(d):
            peer = lax.rem(me + d, n)
            copy_to(step, source.at[peer if spread else me], target, me, peer).start()

    def receive_all(step, target):
        @pl.loop(1, n)
        def _(d):
            peer = lax.rem(me + d, n)
            copy_to(step, target.at[peer], target, peer, peer).wait_recv()

    def sent_all(step, source, spread):
        @pl.loop(1, n)
        def _(d):
            peer = lax.rem(me + d, n)
            src = source.at[peer if spread else me]
            pltpu.make_async_remote_copy(
                src_ref=src,
                dst_ref=src,
                send_sem=send_sem.at[step, peer],
                recv_sem=recv_sem.at[step, peer],
                device_id={"seq": peer},
                device_id_type=MESH,
            ).wait_send()

    wide[...] = picked[...].astype(F32) * inside[...]
    mean_square = jnp.sum(wide[...] * wide[...], axis=1, keepdims=True) / width
    normed = (wide[...] * lax.rsqrt(mean_square + NORM_EPS) * gain_one[...].astype(F32)[None, :]).astype(BF16)
    heads_out = jnp.concatenate([wide[...], normed.astype(F32)], axis=0)
    for j in range(n):
        rows_out[j] = heads_out[:, j * cols : (j + 1) * cols].astype(BF16)
    part_out[...] = jnp.zeros_like(part_out)
    pl.semaphore_wait(barrier, n - 1)
    send_all(0, rows_out, rows_in, True)
    rows_in[me] = rows_out[me]
    receive_all(0, rows_in)
    rows = lax.fori_loop(
        1, n, lambda j, acc: acc + rows_in[j].astype(F32), rows_in[0].astype(F32)
    )
    stream = rows[:tokens]
    normed_local = rows[tokens:].astype(BF16)

    loads[0].wait()
    chunk = 4

    @pl.loop(0, joint_heads // chunk, unroll=True)
    def _(c):
        part = jnp.dot(
            normed_local,
            w_qkv[:, pl.ds(pl.multiple_of(c * (chunk * HEAD_DIM), HEAD_DIM), chunk * HEAD_DIM)],
            preferred_element_type=F32,
        )
        for i in range(chunk):
            h = c * chunk + i
            joint_out[h // joint_each, h % joint_each] = part[:, i * HEAD_DIM : (i + 1) * HEAD_DIM]

    for h in range(joint_heads, n * joint_each):
        joint_out[h // joint_each, h % joint_each] = jnp.zeros((tokens, HEAD_DIM), F32)
    send_all(1, joint_out, joint_in, True)
    joint_in[me] = joint_out[me]
    receive_all(1, joint_in)
    joint = lax.fori_loop(1, n, lambda j, acc: acc + joint_in[j], joint_in[0])
    tiles = []
    for i in range(joint_each):
        h = jnp.minimum(me * joint_each + i, joint_heads - 1)
        x = (joint[i] + bias[pl.ds(h, 1), :]).astype(BF16).astype(F32)
        turned = x * cos[...] + pltpu.roll(x, HEAD_DIM // 2, 1) * sin[...]
        is_key = jnp.full(x.shape, h, jnp.int32) < HEADS + KV_HEADS
        tiles.append(jnp.where(is_key, turned, x))
    heads_all[me] = jnp.concatenate(tiles, axis=0).astype(BF16)
    send_all(2, heads_all, heads_all, False)
    receive_all(2, heads_all)
    rows_each = joint_each * tokens

    @pl.loop(0, n)
    def _(j):
        heads_wide[pl.ds(pl.multiple_of(j * rows_each, 8), rows_each), :] = heads_all[j].astype(F32)

    loads[1].wait()
    loads[2].wait()
    group_rows = group * tokens
    places = me * local_len + lax.broadcasted_iota(jnp.int32, (1, local_len), 1)
    lane = lax.broadcasted_iota(jnp.int32, (tokens, HEAD_DIM), 1)

    exponent = scale / math.log(2.0)

    @pl.loop(0, KV_HEADS)
    def _(k):
        head_cols = pl.ds(pl.multiple_of(k * HEAD_DIM, HEAD_DIM), HEAD_DIM)
        half = group_rows // batches
        for b in range(batches):
            own_rows = pl.ds(b, half, stride=batches)
            q = heads_wide[pl.ds(k * group_rows + b, half, stride=batches), :].astype(BF16)
            scores = lax.dot_general(
                q, keys[b, :, head_cols], (((1,), (1,)), ((), ())), preferred_element_type=F32
            )
            masked = jnp.where(places < lengths[b], scores, MASKED)
            own_top = jnp.max(masked, axis=1, keepdims=True)
            weight = jnp.exp2((masked - own_top) * exponent)
            own_total = jnp.sum(weight, axis=1, keepdims=True)
            own_sum = jnp.dot(
                weight.astype(BF16), values[b, :, head_cols], preferred_element_type=F32
            )
            group_sum[own_rows, :] = own_sum
            group_top[own_rows, :] = jnp.broadcast_to(own_top * scale, own_sum.shape)
            group_total[own_rows, :] = jnp.broadcast_to(own_total, own_sum.shape)
        summed, top, total = group_sum[...], group_top[...], group_total[...]
        for g in range(group):
            h = k * group + g
            owner, slot = h // head_each, h % head_each
            mine = slice(g * tokens, (g + 1) * tokens)
            part_out[owner, slot] = summed[mine]
            stats = part_out[owner, head_each]
            stats = jnp.where(lane == 2 * slot, top[mine], stats)
            part_out[owner, head_each] = jnp.where(lane == 2 * slot + 1, total[mine], stats)

    send_all(3, part_out, part_in, True)
    part_in[me] = part_out[me]

    row = lax.broadcasted_iota(jnp.int32, (tokens, 1), 0)
    fresh = []
    for i in range(head_each):
        h = jnp.minimum(me * head_each + i, HEADS - 1)
        kv = h // group
        q = heads_wide[pl.ds(pl.multiple_of(h * tokens, 8), tokens), :]
        new_key = heads_wide[pl.ds(pl.multiple_of((HEADS + kv) * tokens, 8), tokens), :]
        new_value = heads_wide[
            pl.ds(pl.multiple_of((HEADS + KV_HEADS + kv) * tokens, 8), tokens), :
        ]
        scores = []
        top = jnp.full((tokens, 1), MASKED, F32)
        for t in range(tokens):
            seen = (row % batches == t % batches) & (row >= t)
            score = jnp.sum(q * new_key[t : t + 1], axis=1, keepdims=True) * scale
            score = jnp.where(seen, score, MASKED)
            scores.append((seen, score))
            top = jnp.maximum(top, score)
        fresh.append((top, scores, new_value))

    receive_all(3, part_in)
    tiles = []
    for i in range(head_each):
        top, scores, new_value = fresh[i]

        def stat(j, which):
            return jnp.broadcast_to(
                part_in[j, head_each][:, 2 * i + which : 2 * i + which + 1], (tokens, HEAD_DIM)
            )

        top = jnp.broadcast_to(top, (tokens, HEAD_DIM))
        top = lax.fori_loop(0, n, lambda j, m: jnp.maximum(m, stat(j, 0)), top, unroll=True)
        total = jnp.zeros((tokens, HEAD_DIM), F32)
        summed = jnp.zeros((tokens, HEAD_DIM), F32)
        for t in range(tokens):
            seen, score = scores[t]
            weight = jnp.where(seen, jnp.exp(score - top), 0.0)
            total += weight
            summed += weight.astype(BF16).astype(F32) * new_value[t : t + 1]

        def merge(j, state):
            total, summed = state
            factor = jnp.exp(stat(j, 0) - top)
            return total + stat(j, 1) * factor, summed + part_in[j, i] * factor

        total, summed = lax.fori_loop(0, n, merge, (total, summed), unroll=True)
        tiles.append(summed / total)
    attended_all[me] = jnp.concatenate(tiles, axis=0).astype(BF16)
    send_all(4, attended_all, attended_all, False)
    receive_all(4, attended_all)
    for h in range(HEADS):
        at = (h % head_each) * tokens
        wide[:, h * HEAD_DIM : (h + 1) * HEAD_DIM] = attended_all[h // head_each].astype(F32)[
            at : at + tokens
        ]
    narrow[...] = wide[...].astype(BF16)
    attended_ref[...] = narrow[...]

    loads[3].wait()
    depth = 512

    def piece(c):
        return pl.ds(pl.multiple_of(c * depth, depth), depth)

    mid = stream + lax.fori_loop(
        0,
        width // depth,
        lambda c, acc: acc
        + lax.dot_general(
            narrow[:, piece(c)],
            w_out[:, piece(c)],
            (((1,), (1,)), ((), ())),
            preferred_element_type=F32,
        ),
        jnp.zeros((tokens, cols), F32),
        unroll=True,
    )
    mid_all[me] = mid
    send_all(5, mid_all, mid_all, False)
    receive_all(5, mid_all)
    for j in range(n):
        wide[:, j * cols : (j + 1) * cols] = mid_all[j]
    mean_square = jnp.sum(wide[...] * wide[...], axis=1, keepdims=True) / width
    narrow[...] = (wide[...] * lax.rsqrt(mean_square + NORM_EPS) * gain_two[...].astype(F32)[None, :]).astype(BF16)

    loads[4].wait()
    loads[5].wait()
    units = w_gate.shape[1]

    def both(c, state):
        gate, upper = state
        x = narrow[:, piece(c)]
        return (
            gate + jnp.dot(x, w_gate[piece(c), :], preferred_element_type=F32),
            upper + jnp.dot(x, w_up[piece(c), :], preferred_element_type=F32),
        )

    zero = jnp.zeros((tokens, units), F32)
    gate, upper = lax.fori_loop(0, width // depth, both, (zero, zero), unroll=True)
    hidden = (gate / (1.0 + jnp.exp(-gate)) * upper).astype(BF16)
    loads[6].wait()

    @pl.loop(0, width // depth, unroll=True)
    def _(c):
        wide[:, piece(c)] = jnp.dot(hidden, w_down[:, piece(c)], preferred_element_type=F32)

    for j in range(n):
        down_out[j] = wide[:, j * cols : (j + 1) * cols]
    send_all(6, down_out, down_in, True)
    down_in[me] = down_out[me]
    receive_all(6, down_in)
    summed = lax.fori_loop(1, n, lambda j, acc: acc + down_in[j], down_in[0])
    layer_ref[...] = (mid + summed).astype(BF16)

    sent_all(0, rows_out, True)
    sent_all(1, joint_out, True)
    sent_all(2, heads_all, False)
    sent_all(3, part_out, True)
    sent_all(4, attended_all, False)
    sent_all(5, mid_all, False)
    sent_all(6, down_out, True)


def body(
    token_ids,
    lengths,
    embed_table,
    attn_gain,
    w_qkv,
    qkv_bias,
    cache_keys,
    cache_values,
    w_out,
    mlp_gain,
    w_gate,
    w_up,
    w_down,
):
    n = lax.axis_size("seq")
    rank = lax.axis_index("seq")
    step_count, batch_count = token_ids.shape
    tokens = step_count * batch_count
    width = embed_table.shape[1]
    vocab_rows = embed_table.shape[0]
    cols = w_out.shape[1]
    local_ids = token_ids.reshape(-1) - rank * vocab_rows
    inside = (local_ids >= 0) & (local_ids < vocab_rows)
    picked = embed_table.at[jnp.clip(local_ids, 0, vocab_rows - 1)].get(mode="promise_in_bounds")
    positions = (lengths[None, :] + jnp.arange(step_count, dtype=jnp.int32)[:, None]).reshape(-1)
    half = HEAD_DIM // 2
    frequency = ROPE_BASE ** (-2.0 * jnp.arange(half, dtype=F32) / HEAD_DIM)
    angles = positions.astype(F32)[:, None] * frequency
    cosine, sine = jnp.cos(angles), jnp.sin(angles)
    cos = jnp.concatenate([cosine, cosine], axis=1)
    sin = jnp.concatenate([-sine, sine], axis=1)
    joint_heads = HEADS + 2 * KV_HEADS
    joint_each = -(-joint_heads // n)
    head_each = -(-HEADS // n)
    vmem = pl.BlockSpec(memory_space=pltpu.VMEM)
    hbm = pl.BlockSpec(memory_space=pl.ANY)
    attended, layer_out = pl.pallas_call(
        functools.partial(layer_kernel, n),
        out_shape=(
            jax.ShapeDtypeStruct((tokens, width), BF16),
            jax.ShapeDtypeStruct((tokens, cols), BF16),
        ),
        in_specs=[pl.BlockSpec(memory_space=pltpu.SMEM)] + [vmem] * 7 + [hbm] * 7,
        out_specs=(vmem, vmem),
        scratch_shapes=[
            pltpu.VMEM(a.shape, a.dtype)
            for a in (w_qkv, cache_keys, cache_values, w_out.T, w_gate, w_up, w_down)
        ]
        + [
            pltpu.VMEM((n, 2 * tokens, cols), BF16),
            pltpu.VMEM((n, 2 * tokens, cols), BF16),
            pltpu.VMEM((n, joint_each, tokens, HEAD_DIM), F32),
            pltpu.VMEM((n, joint_each, tokens, HEAD_DIM), F32),
            pltpu.VMEM((n, joint_each * tokens, HEAD_DIM), BF16),
            pltpu.VMEM((n * joint_each * tokens, HEAD_DIM), F32),
            pltpu.VMEM((n, head_each + 1, tokens, HEAD_DIM), F32),
            pltpu.VMEM((n, head_each + 1, tokens, HEAD_DIM), F32),
            pltpu.VMEM((n, head_each * tokens, HEAD_DIM), BF16),
            pltpu.VMEM((n, tokens, cols), F32),
            pltpu.VMEM((tokens, width), F32),
            pltpu.VMEM((tokens, width), BF16),
            pltpu.VMEM((n, tokens, cols), F32),
            pltpu.VMEM((n, tokens, cols), F32),
            pltpu.VMEM((HEADS // KV_HEADS * tokens, HEAD_DIM), F32),
            pltpu.VMEM((HEADS // KV_HEADS * tokens, HEAD_DIM), F32),
            pltpu.VMEM((HEADS // KV_HEADS * tokens, HEAD_DIM), F32),
            pltpu.SemaphoreType.DMA((7,)),
            pltpu.SemaphoreType.DMA((7, n)),
            pltpu.SemaphoreType.DMA((7, n)),
        ],
        compiler_params=pltpu.CompilerParams(
            collective_id=0, has_side_effects=True, vmem_limit_bytes=67043328
        ),
    )(
        lengths,
        picked,
        inside.astype(F32)[:, None],
        attn_gain,
        qkv_bias.reshape(joint_heads, HEAD_DIM),
        cos,
        sin,
        mlp_gain,
        w_qkv,
        cache_keys,
        cache_values,
        w_out.T,
        w_gate,
        w_up,
        w_down,
    )
    return (
        attended.reshape(step_count, batch_count, width),
        layer_out.reshape(step_count, batch_count, cols),
    )


def solution(mesh):
    return jax.shard_map(
        body,
        mesh=mesh,
        in_specs=(
            P(None, "parts"),
            P("parts"),
            P("seq", None),
            P(),
            P("seq", None),
            P(),
            P("parts", "seq", None),
            P("parts", "seq", None),
            P(None, "seq"),
            P(),
            P(None, "seq"),
            P(None, "seq"),
            P("seq", None),
        ),
        out_specs=(P(None, "parts", None), P(None, "parts", "seq")),
        check_vma=False,
    )
```
